512 devices in a mesh: groups: 2 (over y), ctx: 16 (over z), seq: 8 (over x), head: 2 (over core).
Axes of the slice: x: 8, y: 2, z: 16, core: 2. Of those that a mesh axis runs over, the one named last changes fastest.
The devices are a block of a 8x8x16 slice.
Arguments:
- queries: bfloat16 [16, 4, 128, 576], P(('groups', 'seq'), None, ('ctx', 'head')), parts along dimension 0, may hold values from -36 to 36
- cache: bfloat16 [16, 49152, 576], P(('groups', 'seq'), 'ctx'), parts along dimension 0, may hold values from -8 to 8
- lengths: int32 [16], P(('groups', 'seq')), parts along dimension 0, may hold values from 12288 to 49152, as said below
- offsets: int32 [16, 4], P(('groups', 'seq')), parts along dimension 0, may hold values from 0 to 3
- w_uv: bfloat16 [128, 512, 128], P(('ctx', 'head')), may hold values from -0.25 to 0.25
- w_out: bfloat16 [16384, 7168], P(('ctx', 'head'), 'seq'), may hold values from -0.046875 to 0.046875
Outputs:
- mixed: bfloat16 [64, 7168], P(('groups', 'ctx', 'head'), 'seq'), parts along dimension 0
The draws below stay inside these ranges and needn't reach their ends.
There are 2 independent parts, one for each index of `groups`. The reference program is written for one: setup_inputs(seed, part) draws one part's arguments, and reference() takes and returns one part's arrays. A program takes and returns all parts, laid end to end along the dimension named above; an argument that names none is the same for every part. Nothing has to cross between parts.
Inputs may be any that keep to these rules, and one draw needn't show every extreme that they name: `lengths`: each sequence's filled length, its 4 draft tokens included; some sequence reaches 49152 in every draw. Draft token t of sequence s sits at position lengths[s] - 4 + offsets[s, t].
All inputs are finite; a program needn't handle non-finite values.
Results may differ from the reference program's by a relative error of at most 0.014.
Values may be sent and summed in bfloat16 or wider, within the bound.
No kernel may reach another device: no remote copies, remote signals or barrier semaphores. Data moves between devices by JAX's collectives and lax.ppermute only.
A program may use at most 64 MiB of HBM per device.

```python
import jax
import jax.numpy as jnp
from jax import lax

D = 7168
HEADS = 128
LATENT = 512
ROPE = 64
NOPE = 128
VDIM = 128
DRAFT = 4
SEQS = 8
LEN = 49152


def draw_cache(key, part):
    entries = LATENT + ROPE
    values = jnp.clip(jax.random.normal(jax.random.fold_in(key, 11), (SEQS, LEN, entries)), -4.5, 4.5)
    return values.astype(jnp.bfloat16)


def draw_queries(key, part):
    shape_all = (SEQS, DRAFT, HEADS, LATENT + ROPE)
    values = 2.0 * jnp.clip(jax.random.normal(jax.random.fold_in(key, 12), shape_all), -4.0, 4.0)
    return values.astype(jnp.bfloat16)


def draw_lengths(key, part):
    own_key = jax.random.fold_in(key, part)
    values = jax.random.randint(jax.random.fold_in(own_key, 21), (SEQS,), LEN // 4, LEN + 1)
    longest = jax.random.randint(jax.random.fold_in(own_key, 22), (), 0, SEQS)
    return jnp.where(jnp.arange(SEQS, dtype=jnp.int32) == longest, LEN, values).astype(jnp.int32)


def touch_ends(values, stream_key, low, top_value):
    place = [jax.random.randint(jax.random.fold_in(stream_key, axis), (), 0, length) for axis, length in enumerate(values.shape)]
    widest = values.shape.index(max(values.shape))
    neighbour = place[:widest] + [(place[widest] + 1) % values.shape[widest]] + place[widest + 1:]
    return values.at[tuple(place)].set(low).at[tuple(neighbour)].set(top_value)


def level_of(rng, dims, shards, smallest, largest):
    level = 1.0
    for dim, blocks in shards:
        heights = jax.random.uniform(jax.random.fold_in(jax.random.fold_in(rng, 6), dim), (blocks,), jnp.float32, smallest / len(shards), largest / len(shards))
        level = level * jnp.repeat(jnp.exp(heights), dims[dim] // blocks).reshape((-1,) + (1,) * (len(dims) - 1 - dim))
    return level


def noise(key, dims, width, bound, split=(), held_as=jnp.bfloat16):
    factor_of = level_of(key, dims, split, -0.22, 0.18) if split else 1.0
    drawn = jax.random.normal(key, dims, jnp.float32) * width * factor_of
    return jnp.minimum(jnp.maximum(drawn, -bound), bound).astype(held_as)


def setup_inputs(seed: int = 0, part: int = 0) -> dict:
    seeds = jax.random.split(jax.random.key(seed), 7)
    own_keys = jax.random.split(jax.random.fold_in(seeds[6], part), 7)
    return {
        "queries": draw_queries(jax.random.fold_in(jax.random.fold_in(seeds[6], part), 71), part),
        "cache": draw_cache(jax.random.fold_in(jax.random.fold_in(seeds[6], part), 71), part),
        "lengths": draw_lengths(jax.random.fold_in(jax.random.fold_in(seeds[6], part), 71), part),
        "offsets": touch_ends(jax.random.randint(own_keys[3], (SEQS, DRAFT), 0, DRAFT), jax.random.fold_in(own_keys[3], 1), 0, DRAFT - 1).astype(jnp.int32),
        "w_uv": noise(seeds[4], (HEADS, LATENT, VDIM), LATENT ** -0.5, 0.25, ((0, 32),)),
        "w_out": noise(seeds[5], (HEADS * VDIM, D), (HEADS * VDIM) ** -0.5, 0.046875, ((0, 32), (1, 8))),
    }


theta = 10000.0
negative = -1e30


def rotate(queries, positions):
    half_rope = ROPE // 2
    frequency = theta ** (-2.0 * jnp.arange(half_rope, dtype=jnp.float32) / ROPE)
    angles = positions.astype(jnp.float32)[..., None] * frequency
    cosine = jnp.cos(angles)[..., None, :]
    sine_part = jnp.sin(angles)[..., None, :]
    front_half = queries[..., LATENT:LATENT + half_rope].astype(jnp.float32)
    back_half = queries[..., LATENT + half_rope:].astype(jnp.float32)
    turned = jnp.concatenate([front_half * cosine - back_half * sine_part, back_half * cosine + front_half * sine_part], axis=-1)
    return jnp.concatenate([queries[..., :LATENT], turned.astype(jnp.bfloat16)], axis=-1)


def attend(packed):
    rotated, cache_rows, limits = packed
    flattened = rotated.reshape(DRAFT * HEADS, rotated.shape[-1])
    scores = lax.dot_general(flattened, cache_rows, (((1,), (1,)), ((), ())), preferred_element_type=jnp.float32) * (NOPE + ROPE) ** -0.5
    places = jnp.arange(cache_rows.shape[0], dtype=jnp.int32)
    bounds = jnp.repeat(limits, HEADS)
    visible = places[None, :] <= bounds[:, None]
    maxima = jnp.max(jnp.where(visible, scores, negative), axis=1, keepdims=True)
    weights = jnp.where(visible, jnp.exp(scores - maxima), 0.0)
    totals = jnp.sum(weights, axis=1, keepdims=True)
    numerators = jnp.dot(weights.astype(jnp.bfloat16), cache_rows[:, :LATENT], preferred_element_type=jnp.float32)
    return (numerators / totals).astype(jnp.bfloat16).reshape(DRAFT, HEADS, LATENT)


def reference(queries, cache, lengths, offsets, w_uv, w_out):
    positions = (lengths[:, None] - DRAFT + offsets).astype(jnp.int32)
    rotated = rotate(queries, positions)
    attended = lax.map(attend, (rotated, cache, positions))
    head_values = jnp.einsum("sthl,hlv->sthv", attended.astype(jnp.float32), w_uv.astype(jnp.float32)).astype(jnp.bfloat16)
    flattened = head_values.reshape(SEQS * DRAFT, HEADS * VDIM)
    return jnp.dot(flattened, w_out, preferred_element_type=jnp.float32).astype(jnp.bfloat16)
```

```python
import jax
import jax.numpy as jnp
from jax import lax
from jax.sharding import PartitionSpec as P

LATENT = 512
ROPE = 64
NOPE = 128
DRAFT = 4


theta = 10000.0
negative = -1e30


def copy_for_each(value, axis):
    devices = lax.axis_size(axis)
    return lax.all_to_all(
        jnp.broadcast_to(value[None], (devices, *value.shape)), axis, 0, 0, tiled=True
    )


def cut_along(value, dim, devices):
    dims = value.shape
    blocks = value.reshape(*dims[:dim], devices, dims[dim] // devices, *dims[dim + 1 :])
    return jnp.moveaxis(blocks, dim, 0)


def joined_along(blocks, dim):
    blocks = jnp.moveaxis(blocks, 0, dim)
    dims = blocks.shape
    return blocks.reshape(*dims[:dim], dims[dim] * dims[dim + 1], *dims[dim + 2 :])


def collect(value, axis, dim):
    return joined_along(copy_for_each(value, axis), dim)


def rotate(queries, positions):
    half_rope = ROPE // 2
    frequency = theta ** (-2.0 * jnp.arange(half_rope, dtype=jnp.float32) / ROPE)
    angles = positions.astype(jnp.float32)[..., None] * frequency
    cosine = jnp.cos(angles)[..., None, :]
    sine_part = jnp.sin(angles)[..., None, :]
    front_half = queries[..., LATENT : LATENT + half_rope].astype(jnp.float32)
    back_half = queries[..., LATENT + half_rope :].astype(jnp.float32)
    turned = jnp.concatenate(
        [front_half * cosine - back_half * sine_part, back_half * cosine + front_half * sine_part],
        axis=-1,
    )
    return jnp.concatenate([queries[..., :LATENT], turned.astype(jnp.bfloat16)], axis=-1)


def score_rows(blocks, limits, cache_rows, first_place):
    scores = lax.dot_general(
        blocks, cache_rows, (((1,), (1,)), ((), ())), preferred_element_type=jnp.float32
    ) * (NOPE + ROPE) ** (-0.5)
    places = first_place + jnp.arange(cache_rows.shape[0], dtype=jnp.int32)
    visible = places[None, :] <= limits[:, None]
    return (scores, visible)


def in_pieces(value, count):
    pieces = []
    for _ in range(count):
        piece = lax.reduce_precision(value, 8, 7)
        pieces.append(piece.astype(jnp.bfloat16))
        value = value - piece
    return jnp.stack(pieces, axis=-1)


def per_device(queries, cache, lengths, offsets, w_uv, w_out):
    head_count = queries.shape[2]
    entries = queries.shape[3]
    positions = lengths[0] - DRAFT + offsets[0]
    rotated = rotate(queries[0], positions)
    cache_rows = cache[0]
    values = cache_rows[:, :LATENT]
    first_place = lax.axis_index("ctx") * cache_rows.shape[0]
    devices_ctx = lax.axis_size("ctx")
    rows = DRAFT * head_count
    blocks = rotated.reshape(rows, entries)
    gathered = copy_for_each(blocks, "ctx").reshape(devices_ctx * rows, entries)
    limits = jnp.tile(jnp.repeat(positions, head_count), devices_ctx)
    scores, visible = score_rows(gathered, limits, cache_rows, first_place)
    maxima = jnp.max(jnp.where(visible, scores, negative), axis=1)
    weights = jnp.where(visible, jnp.exp(scores - maxima[:, None]), 0.0)
    totals = jnp.sum(weights, axis=1)
    numerators = jnp.dot(weights.astype(jnp.bfloat16), values, preferred_element_type=jnp.float32)
    shares = numerators / jnp.maximum(totals, 1.0)[:, None]
    stats = jnp.concatenate([in_pieces(maxima, 3), in_pieces(totals, 3)], axis=-1)
    sent = jnp.concatenate([shares.astype(jnp.bfloat16), stats], axis=-1)
    sent = sent.reshape(devices_ctx, rows, LATENT + 6)
    arrived = lax.all_to_all(sent, "ctx", split_axis=0, concat_axis=0, tiled=True)
    arrived = arrived.astype(jnp.float32)
    peaks = arrived[..., LATENT : LATENT + 3].sum(axis=-1)
    parts = arrived[..., LATENT + 3 :].sum(axis=-1)
    parts = parts * jnp.exp(peaks - peaks.max(axis=0))
    parts = parts / parts.sum(axis=0)
    attended = (arrived[..., :LATENT] * parts[..., None]).sum(axis=0)
    attended = attended.astype(jnp.bfloat16).reshape(DRAFT, head_count, LATENT)
    head_values = jnp.einsum(
        "thl,hlv->thv", attended, w_uv, preferred_element_type=jnp.float32
    ).astype(jnp.bfloat16)
    head_values = head_values.reshape(DRAFT, head_count * head_values.shape[2])
    every_token = collect(head_values, "seq", 0)
    mixed = jnp.dot(every_token, w_out, preferred_element_type=jnp.float32).astype(jnp.bfloat16)
    mixed = cut_along(mixed, 0, lax.axis_size(("ctx", "head")))
    mixed = lax.all_to_all(mixed, ("ctx", "head"), split_axis=0, concat_axis=0, tiled=True)
    return mixed.astype(jnp.float32).sum(axis=0).astype(jnp.bfloat16)


def solution(mesh):
    in_specs = (
        P(("groups", "seq"), None, ("ctx", "head"), None),
        P(("groups", "seq"), "ctx", None),
        P(("groups", "seq")),
        P(("groups", "seq"), None),
        P(("ctx", "head"), None, None),
        P(("ctx", "head"), "seq"),
    )
    out_specs = P(("groups", "ctx", "head"), "seq")
    return jax.shard_map(
        per_device, mesh=mesh, in_specs=in_specs, out_specs=out_specs, check_vma=False
    )
```

```python
import functools
import math

import jax
import jax.numpy as jnp
import numpy as np
from jax import lax
from jax.experimental import pallas as pl
from jax.experimental.pallas import tpu as pltpu
from jax.sharding import PartitionSpec as P

LATENT = 512
ROPE = 64
NOPE = 128
DRAFT = 4
LANES = 128
TILE = 256

theta = 10000.0
negative = -1e30
scale = (NOPE + ROPE) ** (-0.5)
scale_log2 = scale * math.log2(math.e)

F32 = jnp.float32
BF16 = jnp.bfloat16
VMEM = pl.BlockSpec(memory_space=pltpu.VMEM)
SMEM = pl.BlockSpec(memory_space=pltpu.SMEM)
LATENT_BLOCKS = LATENT // LANES


def packed_angles(positions, rows):
    half = ROPE // 2
    frequency = np.float32(theta ** (-2.0 * np.arange(half) / ROPE))
    by_row = jnp.repeat(positions.astype(F32), rows // DRAFT).reshape(2, rows // 2)
    angles = by_row[:, :, None] * jnp.asarray(np.tile(frequency, 2))
    return jnp.concatenate([angles[0], angles[1]], axis=-1)


def rotation_tables(positions, rows):
    angles = packed_angles(positions, rows)
    lane = lax.broadcasted_iota(jnp.int32, angles.shape, 1)
    sign = jnp.where(lane % ROPE < ROPE // 2, -1.0, 1.0).astype(F32)
    return jnp.stack([jnp.cos(angles), jnp.sin(angles) * sign])


def pack_kernel(queries_ref, sent_ref):
    rows = jnp.concatenate([queries_ref[0, t].astype(F32) for t in range(DRAFT)], axis=0)
    half = rows.shape[0] // 2
    parts = [rows[:, j * LANES : (j + 1) * LANES] for j in range(LATENT_BLOCKS)]
    rope = rows[:, LATENT : LATENT + ROPE]
    parts.append(jnp.concatenate([rope[:half], rope[half:]], axis=1))
    message = jnp.concatenate(parts, axis=0).astype(BF16)
    for d in range(sent_ref.shape[0]):
        sent_ref[d] = message


def pieces_of(value):
    first = value.astype(BF16).astype(F32)
    second = (value - first).astype(BF16).astype(F32)
    third = (value - first - second).astype(BF16).astype(F32)
    return first, second, third


def attend_kernel(scalars_ref, tables_ref, arrived_ref, cache_ref, sent_ref, q_ref, s_ref, p_ref):
    devices = arrived_ref.shape[0]
    places = cache_ref.shape[0]
    rows = q_ref.shape[0] // devices
    half = rows // 2
    for j in range(LATENT_BLOCKS):
        block = arrived_ref[:, j * rows : (j + 1) * rows, :]
        q_ref[:, j * LANES : (j + 1) * LANES] = block.reshape(devices * rows, LANES)
    x = arrived_ref[:, LATENT_BLOCKS * rows :, :].astype(F32).reshape(devices * half, LANES)
    lane = lax.broadcasted_iota(jnp.int32, x.shape, 1)
    partner = jnp.where(
        lane % ROPE < ROPE // 2,
        pltpu.roll(x, LANES - ROPE // 2, 1),
        pltpu.roll(x, ROPE // 2, 1),
    )
    shape3 = (devices, half, LANES)
    turned = x.reshape(shape3) * tables_ref[0][None] + partner.reshape(shape3) * tables_ref[1][None]
    swapped = pltpu.roll(turned.reshape(devices * half, LANES), ROPE, 1).reshape(shape3)
    rope = jnp.stack([turned, swapped], axis=1).reshape(devices * rows, LANES)
    q_ref[:, LATENT:] = rope[:, :ROPE].astype(BF16)

    row = lax.broadcasted_iota(jnp.int32, (devices * rows, TILE), 0) % rows
    limits = jnp.full(row.shape, scalars_ref[0], jnp.int32)
    for t in range(1, DRAFT):
        limits = jnp.where(row >= t * (rows // DRAFT), scalars_ref[t], limits)
    limits = limits - lax.broadcasted_iota(jnp.int32, row.shape, 1)
    top = jnp.full((devices * rows, LANES), negative, F32)
    for i in range(places // TILE):
        scores = lax.dot_general(
            q_ref[...],
            cache_ref[i * TILE : (i + 1) * TILE, :],
            (((1,), (1,)), ((), ())),
            preferred_element_type=F32,
        )
        scores = jnp.where(limits >= i * TILE, scores, negative)
        s_ref[:, i * TILE : (i + 1) * TILE] = scores
        for j in range(TILE // LANES):
            top = jnp.maximum(top, scores[:, j * LANES : (j + 1) * LANES])
    peak = jnp.max(top, axis=1, keepdims=True)
    total = jnp.zeros((devices * rows, LANES), F32)
    for i in range(places // TILE):
        weights = jnp.exp2((s_ref[:, i * TILE : (i + 1) * TILE] - peak) * scale_log2)
        for j in range(TILE // LANES):
            total += weights[:, j * LANES : (j + 1) * LANES]
        p_ref[:, i * TILE : (i + 1) * TILE] = weights.astype(BF16)
    total = jnp.sum(total, axis=1, keepdims=True)
    share = jnp.dot(p_ref[...], cache_ref[:, :LATENT], preferred_element_type=F32) / total
    for j in range(LATENT_BLOCKS):
        block = share[:, j * LANES : (j + 1) * LANES].astype(BF16)
        sent_ref[:, j * rows : (j + 1) * rows, :] = block.reshape(devices, rows, LANES)
    lane = lax.broadcasted_iota(jnp.int32, (devices * rows, LANES), 1)
    stats = jnp.zeros(lane.shape, F32)
    for k, piece in enumerate((*pieces_of(peak), *pieces_of(total))):
        stats = jnp.where(lane % ROPE == k, piece, stats)
    stats = stats.reshape(devices, 2, half, LANES)
    lane = lax.broadcasted_iota(jnp.int32, (devices, half, LANES), 2)
    sent_ref[:, LATENT_BLOCKS * rows :, :] = jnp.where(
        lane < ROPE, stats[:, 0], stats[:, 1]
    ).astype(BF16)


def combine_kernel(arrived_ref, w_uv_ref, sent_ref):
    devices, _, _ = arrived_ref.shape
    heads = w_uv_ref.shape[0]
    rows = DRAFT * heads
    half = rows // 2
    packed = arrived_ref[:, LATENT_BLOCKS * rows :, :].astype(F32)
    stats = jnp.concatenate(
        [packed, pltpu.roll(packed.reshape(devices * half, LANES), ROPE, 1).reshape(packed.shape)],
        axis=1,
    )
    peaks = stats[:, :, 0:1] + stats[:, :, 1:2] + stats[:, :, 2:3]
    parts = stats[:, :, 3:4] + stats[:, :, 4:5] + stats[:, :, 5:6]
    parts = parts * jnp.exp2((peaks - jnp.max(peaks, axis=0, keepdims=True)) * scale_log2)
    parts = parts / jnp.sum(parts, axis=0, keepdims=True)
    blocks = []
    for j in range(LATENT_BLOCKS):
        block = arrived_ref[:, j * rows : (j + 1) * rows, :].astype(F32)
        blocks.append(jnp.sum(block * parts, axis=0))
    attended = jnp.concatenate(blocks, axis=1).astype(BF16)
    row = lax.broadcasted_iota(jnp.int32, (rows, w_uv_ref.shape[2]), 0)
    values = []
    for h in range(heads):
        value = jnp.dot(attended, w_uv_ref[h], preferred_element_type=F32)
        values.append(jnp.where(row % heads == h, value, 0.0))
    values = jnp.concatenate(values, axis=1).astype(BF16)
    token = lax.broadcasted_iota(jnp.int32, (DRAFT, rows), 0)
    member = lax.broadcasted_iota(jnp.int32, (DRAFT, rows), 1) // heads
    pick = (token == member).astype(BF16)
    values = jnp.dot(pick, values, preferred_element_type=F32).astype(BF16)
    for d in range(sent_ref.shape[0]):
        sent_ref[d] = values


def per_device(queries, cache, lengths, offsets, w_uv, w_out):
    heads = queries.shape[2]
    rows = DRAFT * heads
    places = cache.shape[1]
    devices_ctx = lax.axis_size("ctx")
    devices_seq = lax.axis_size("seq")
    message = LATENT_BLOCKS * rows + rows // 2
    positions = lengths[0] - DRAFT + offsets[0]
    sent = pl.pallas_call(
        pack_kernel,
        out_shape=jax.ShapeDtypeStruct((devices_ctx, message, LANES), BF16),
        in_specs=[VMEM],
        out_specs=VMEM,
        name="pack",
    )(queries)
    arrived = lax.all_to_all(sent, "ctx", 0, 0, tiled=True)
    scalars = positions - lax.axis_index("ctx") * places
    all_rows = devices_ctx * rows
    sent = pl.pallas_call(
        attend_kernel,
        out_shape=jax.ShapeDtypeStruct((devices_ctx, message, LANES), BF16),
        in_specs=[SMEM, VMEM, VMEM, VMEM],
        out_specs=VMEM,
        scratch_shapes=[
            pltpu.VMEM((all_rows, LATENT + ROPE), BF16),
            pltpu.VMEM((all_rows, places), F32),
            pltpu.VMEM((all_rows, places), BF16),
        ],
        compiler_params=pltpu.CompilerParams(vmem_limit_bytes=24 * 1024 * 1024),
        name="attend",
    )(scalars, rotation_tables(positions, rows), arrived, cache[0])
    arrived = lax.all_to_all(sent, "ctx", 0, 0, tiled=True)
    sent = pl.pallas_call(
        combine_kernel,
        out_shape=jax.ShapeDtypeStruct((devices_seq, DRAFT, heads * w_uv.shape[2]), BF16),
        in_specs=[VMEM, VMEM],
        out_specs=VMEM,
        name="combine",
    )(arrived, w_uv)
    every_token = lax.all_to_all(sent, "seq", 0, 0, tiled=True)
    every_token = every_token.reshape(devices_seq * DRAFT, w_out.shape[0])
    mixed = jnp.dot(every_token, w_out, preferred_element_type=F32).astype(BF16)
    mixed = lax.all_to_all(mixed[:, None, :], ("ctx", "head"), 0, 0, tiled=True)
    return mixed.astype(F32).sum(axis=0).astype(BF16)


def solution(mesh):
    in_specs = (
        P(("groups", "seq"), None, ("ctx", "head"), None),
        P(("groups", "seq"), "ctx", None),
        P(("groups", "seq")),
        P(("groups", "seq"), None),
        P(("ctx", "head"), None, None),
        P(("ctx", "head"), "seq"),
    )
    out_specs = P(("groups", "ctx", "head"), "seq")
    return jax.shard_map(
        per_device, mesh=mesh, in_specs=in_specs, out_specs=out_specs, check_vma=False
    )
```

```python
import functools
import math

import jax
import jax.numpy as jnp
import numpy as np
from jax import lax
from jax.experimental import pallas as pl
from jax.experimental.pallas import tpu as pltpu
from jax.sharding import PartitionSpec as P

LATENT = 512
ROPE = 64
NOPE = 128
DRAFT = 4
LANES = 128
TILE = 256
COVER = 1 << 24

theta = 10000.0
negative = -1e30
scale = (NOPE + ROPE) ** (-0.5)
scale_log2 = scale * math.log2(math.e)

F32 = jnp.float32
BF16 = jnp.bfloat16
VMEM = pl.BlockSpec(memory_space=pltpu.VMEM)
SMEM = pl.BlockSpec(memory_space=pltpu.SMEM)
LATENT_BLOCKS = LATENT // LANES


def packed_angles(positions, rows):
    half = ROPE // 2
    frequency = np.float32(theta ** (-2.0 * np.arange(half) / ROPE))
    by_row = jnp.repeat(positions.astype(F32), rows // DRAFT).reshape(2, rows // 2)
    angles = by_row[:, :, None] * jnp.asarray(np.tile(frequency, 2))
    return jnp.concatenate([angles[0], angles[1]], axis=-1)


def rotation_tables(positions, rows):
    angles = packed_angles(positions, rows)
    return pl.pallas_call(
        tables_kernel,
        out_shape=jax.ShapeDtypeStruct((2, *angles.shape), F32),
        in_specs=[VMEM, VMEM],
        out_specs=VMEM,
        compiler_params=limited(4),
        cost_estimate=pl.CostEstimate(flops=COVER * 1000, bytes_accessed=COVER, transcendentals=0),
        name="tables",
    )(jnp.cos(angles), jnp.sin(angles))


def pack_kernel(queries_ref, sent_ref):
    rows = jnp.concatenate([queries_ref[0, t].astype(F32) for t in range(DRAFT)], axis=0)
    half = rows.shape[0] // 2
    parts = [rows[:, j * LANES : (j + 1) * LANES] for j in range(LATENT_BLOCKS)]
    rope = rows[:, LATENT : LATENT + ROPE]
    parts.append(jnp.concatenate([rope[:half], rope[half:]], axis=1))
    message = jnp.concatenate(parts, axis=0).astype(BF16)
    for d in range(sent_ref.shape[0]):
        sent_ref[d] = message


def tables_kernel(cosine_ref, sine_ref, tables_ref):
    lane = lax.broadcasted_iota(jnp.int32, cosine_ref.shape, 1)
    tables_ref[0] = cosine_ref[...]
    tables_ref[1] = jnp.where(lane % ROPE < ROPE // 2, -sine_ref[...], sine_ref[...])


def pieces_of(value):
    first = value.astype(BF16).astype(F32)
    second = (value - first).astype(BF16).astype(F32)
    third = (value - first - second).astype(BF16).astype(F32)
    return first, second, third


def attend_kernel(scalars_ref, tables_ref, arrived_ref, cache_ref, sent_ref, q_ref, s_ref, p_ref):
    devices = arrived_ref.shape[0]
    places = cache_ref.shape[1]
    rows = q_ref.shape[0] // devices
    half = rows // 2
    for j in range(LATENT_BLOCKS):
        block = arrived_ref[:, j * rows : (j + 1) * rows, :]
        q_ref[:, j * LANES : (j + 1) * LANES] = block.reshape(devices * rows, LANES)
    x = arrived_ref[:, LATENT_BLOCKS * rows :, :].astype(F32).reshape(devices * half, LANES)
    lane = lax.broadcasted_iota(jnp.int32, x.shape, 1)
    partner = jnp.where(
        lane % ROPE < ROPE // 2,
        pltpu.roll(x, LANES - ROPE // 2, 1),
        pltpu.roll(x, ROPE // 2, 1),
    )
    shape3 = (devices, half, LANES)
    turned = x.reshape(shape3) * tables_ref[0][None] + partner.reshape(shape3) * tables_ref[1][None]
    swapped = pltpu.roll(turned.reshape(devices * half, LANES), ROPE, 1).reshape(shape3)
    rope = jnp.stack([turned, swapped], axis=1).reshape(devices * rows, LANES)
    q_ref[:, LATENT:] = rope[:, :ROPE].astype(BF16)

    row = lax.broadcasted_iota(jnp.int32, (devices * rows, TILE), 0) % rows
    limits = jnp.full(row.shape, scalars_ref[0], jnp.int32)
    for t in range(1, DRAFT):
        limits = jnp.where(row >= t * (rows // DRAFT), scalars_ref[t], limits)
    limits = limits - lax.broadcasted_iota(jnp.int32, row.shape, 1)
    top = jnp.full((devices * rows, LANES), negative, F32)
    for i in range(places // TILE):
        scores = lax.dot_general(
            q_ref[...],
            cache_ref[:, i * TILE : (i + 1) * TILE],
            (((1,), (0,)), ((), ())),
            preferred_element_type=F32,
        )
        scores = jnp.where(limits >= i * TILE, scores, negative)
        s_ref[:, i * TILE : (i + 1) * TILE] = scores
        for j in range(TILE // LANES):
            top = jnp.maximum(top, scores[:, j * LANES : (j + 1) * LANES])
    peak = jnp.max(top, axis=1, keepdims=True)
    total = jnp.zeros((devices * rows, LANES), F32)
    for i in range(places // TILE):
        weights = jnp.exp2((s_ref[:, i * TILE : (i + 1) * TILE] - peak) * scale_log2)
        for j in range(TILE // LANES):
            total += weights[:, j * LANES : (j + 1) * LANES]
        p_ref[:, i * TILE : (i + 1) * TILE] = weights.astype(BF16)
    total = jnp.sum(total, axis=1, keepdims=True)
    share = lax.dot_general(
        p_ref[...],
        cache_ref[:LATENT, :],
        (((1,), (1,)), ((), ())),
        preferred_element_type=F32,
    )
    share = share / total
    for j in range(LATENT_BLOCKS):
        block = share[:, j * LANES : (j + 1) * LANES].astype(BF16)
        sent_ref[:, j * rows : (j + 1) * rows, :] = block.reshape(devices, rows, LANES)
    lane = lax.broadcasted_iota(jnp.int32, (devices * rows, LANES), 1)
    stats = jnp.zeros(lane.shape, F32)
    for k, piece in enumerate((*pieces_of(peak), *pieces_of(total))):
        stats = jnp.where(lane % ROPE == k, piece, stats)
    stats = stats.reshape(devices, 2, half, LANES)
    lane = lax.broadcasted_iota(jnp.int32, (devices, half, LANES), 2)
    sent_ref[:, LATENT_BLOCKS * rows :, :] = jnp.where(
        lane < ROPE, stats[:, 0], stats[:, 1]
    ).astype(BF16)


def combine_kernel(arrived_ref, w_uv_ref, sent_ref):
    devices, _, _ = arrived_ref.shape
    heads = w_uv_ref.shape[0]
    rows = DRAFT * heads
    half = rows // 2
    packed = arrived_ref[:, LATENT_BLOCKS * rows :, :].astype(F32)
    stats = jnp.concatenate(
        [packed, pltpu.roll(packed.reshape(devices * half, LANES), ROPE, 1).reshape(packed.shape)],
        axis=1,
    )
    peaks = stats[:, :, 0:1] + stats[:, :, 1:2] + stats[:, :, 2:3]
    parts = stats[:, :, 3:4] + stats[:, :, 4:5] + stats[:, :, 5:6]
    parts = parts * jnp.exp2((peaks - jnp.max(peaks, axis=0, keepdims=True)) * scale_log2)
    parts = parts / jnp.sum(parts, axis=0, keepdims=True)
    blocks = []
    for j in range(LATENT_BLOCKS):
        block = arrived_ref[:, j * rows : (j + 1) * rows, :].astype(F32)
        blocks.append(jnp.sum(block * parts, axis=0))
    attended = jnp.concatenate(blocks, axis=1).astype(BF16)
    row = lax.broadcasted_iota(jnp.int32, (rows, w_uv_ref.shape[2]), 0)
    values = []
    for h in range(heads):
        value = jnp.dot(attended, w_uv_ref[h], preferred_element_type=F32)
        values.append(jnp.where(row % heads == h, value, 0.0))
    values = jnp.concatenate(values, axis=1).astype(BF16)
    token = lax.broadcasted_iota(jnp.int32, (DRAFT, rows), 0)
    member = lax.broadcasted_iota(jnp.int32, (DRAFT, rows), 1) // heads
    pick = (token == member).astype(BF16)
    values = jnp.dot(pick, values, preferred_element_type=F32).astype(BF16)
    for d in range(sent_ref.shape[0]):
        sent_ref[d] = values


def project_kernel(values_ref, w_out_ref, sent_ref):
    devices = values_ref.shape[0]
    blocks = sent_ref.shape[1]
    values = jnp.concatenate([values_ref[d].astype(F32) for d in range(devices)], axis=0)
    mixed = jnp.dot(values.astype(BF16), w_out_ref[...], preferred_element_type=F32)
    width = mixed.shape[1]
    pad = blocks * LANES - width
    mixed = jnp.concatenate([mixed, jnp.zeros((mixed.shape[0], pad), F32)], axis=1)
    sent_ref[...] = mixed.reshape(mixed.shape[0], blocks, LANES).astype(BF16)


def total_kernel(arrived_ref, mixed_ref):
    total = jnp.sum(arrived_ref[...].astype(F32), axis=0)
    for j in range(mixed_ref.shape[1] // LANES):
        mixed_ref[:, j * LANES : (j + 1) * LANES] = total[j : j + 1].astype(BF16)


def limited(mebibytes):
    return pltpu.CompilerParams(vmem_limit_bytes=mebibytes * 1024 * 1024)


def per_device(queries, cache, lengths, offsets, w_uv, w_out):
    heads = queries.shape[2]
    rows = DRAFT * heads
    places = cache.shape[1]
    devices_ctx = lax.axis_size("ctx")
    devices_seq = lax.axis_size("seq")
    message = LATENT_BLOCKS * rows + rows // 2
    positions = lengths[0] - DRAFT + offsets[0]
    sent = pl.pallas_call(
        pack_kernel,
        out_shape=jax.ShapeDtypeStruct((devices_ctx, message, LANES), BF16),
        in_specs=[VMEM],
        out_specs=VMEM,
        compiler_params=limited(4),
        name="pack",
    )(queries)
    arrived = lax.all_to_all(sent, "ctx", 0, 0, tiled=True)
    scalars = positions - lax.axis_index("ctx") * places
    all_rows = devices_ctx * rows
    sent = pl.pallas_call(
        attend_kernel,
        out_shape=jax.ShapeDtypeStruct((devices_ctx, message, LANES), BF16),
        in_specs=[SMEM, VMEM, VMEM, VMEM],
        out_specs=VMEM,
        scratch_shapes=[
            pltpu.VMEM((all_rows, LATENT + ROPE), BF16),
            pltpu.VMEM((all_rows, places), F32),
            pltpu.VMEM((all_rows, places), BF16),
        ],
        compiler_params=limited(24),
        name="attend",
    )(scalars, rotation_tables(positions, rows), arrived, cache[0].T)
    arrived = lax.all_to_all(sent, "ctx", 0, 0, tiled=True)
    sent = pl.pallas_call(
        combine_kernel,
        out_shape=jax.ShapeDtypeStruct((devices_seq, DRAFT, heads * w_uv.shape[2]), BF16),
        in_specs=[VMEM, VMEM],
        out_specs=VMEM,
        compiler_params=limited(8),
        name="combine",
    )(arrived, w_uv)
    every_token = lax.all_to_all(sent, "seq", 0, 0, tiled=True)
    width = w_out.shape[1]
    blocks = -(-width // (LANES * 8)) * 8
    sent = pl.pallas_call(
        project_kernel,
        out_shape=jax.ShapeDtypeStruct((devices_seq * DRAFT, blocks, LANES), BF16),
        in_specs=[VMEM, VMEM],
        out_specs=VMEM,
        compiler_params=limited(8),
        name="project",
    )(every_token, w_out)
    arrived = lax.all_to_all(sent, ("ctx", "head"), 0, 0, tiled=True)
    return pl.pallas_call(
        total_kernel,
        out_shape=jax.ShapeDtypeStruct((1, width), BF16),
        in_specs=[VMEM],
        out_specs=VMEM,
        compiler_params=limited(4),
        name="total",
    )(arrived)


def solution(mesh):
    in_specs = (
        P(("groups", "seq"), None, ("ctx", "head"), None),
        P(("groups", "seq"), "ctx", None),
        P(("groups", "seq")),
        P(("groups", "seq"), None),
        P(("ctx", "head"), None, None),
        P(("ctx", "head"), "seq"),
    )
    out_specs = P(("groups", "ctx", "head"), "seq")
    return jax.shard_map(
        per_device, mesh=mesh, in_specs=in_specs, out_specs=out_specs, check_vma=False
    )
```

```python
import functools
import math

import jax
import jax.numpy as jnp
import numpy as np
from jax import lax
from jax.experimental import pallas as pl
from jax.experimental.pallas import tpu as pltpu
from jax.sharding import PartitionSpec as P

LATENT = 512
ROPE = 64
NOPE = 128
DRAFT = 4
LANES = 128
TILE = 256
COVER = 1 << 24
STAGGER = 1000

theta = 10000.0
negative = -1e30
scale = (NOPE + ROPE) ** (-0.5)
scale_log2 = scale * math.log2(math.e)

F32 = jnp.float32
BF16 = jnp.bfloat16
VMEM = pl.BlockSpec(memory_space=pltpu.VMEM)
SMEM = pl.BlockSpec(memory_space=pltpu.SMEM)
LATENT_BLOCKS = LATENT // LANES


def packed_angles(positions, rows):
    half = ROPE // 2
    frequency = np.float32(theta ** (-2.0 * np.arange(half) / ROPE))
    by_row = jnp.repeat(positions.astype(F32), rows // DRAFT).reshape(2, rows // 2)
    angles = by_row[:, :, None] * jnp.asarray(np.tile(frequency, 2))
    return jnp.concatenate([angles[0], angles[1]], axis=-1)


def rotation_tables(positions, rows):
    angles = packed_angles(positions, rows)
    return pl.pallas_call(
        tables_kernel,
        out_shape=jax.ShapeDtypeStruct((2, *angles.shape), F32),
        in_specs=[VMEM, VMEM],
        out_specs=VMEM,
        compiler_params=limited(4),
        cost_estimate=pl.CostEstimate(flops=COVER * 1000, bytes_accessed=COVER, transcendentals=0),
        name="tables",
    )(jnp.cos(angles), jnp.sin(angles))


def pack_kernel(queries_ref, sent_ref, spun_ref):
    @pl.when(lax.axis_index("head") == 0)
    def _():
        spun_ref[...] = lax.fori_loop(
            0, STAGGER, lambda i, x: x * 0.999 + 0.5, jnp.ones(spun_ref.shape, F32)
        )

    rows = jnp.concatenate([queries_ref[0, t].astype(F32) for t in range(DRAFT)], axis=0)
    half = rows.shape[0] // 2
    parts = [rows[:, j * LANES : (j + 1) * LANES] for j in range(LATENT_BLOCKS)]
    rope = rows[:, LATENT : LATENT + ROPE]
    parts.append(jnp.concatenate([rope[:half], rope[half:]], axis=1))
    message = jnp.concatenate(parts, axis=0).astype(BF16)
    for d in range(sent_ref.shape[0]):
        sent_ref[d] = message


def tables_kernel(cosine_ref, sine_ref, tables_ref):
    lane = lax.broadcasted_iota(jnp.int32, cosine_ref.shape, 1)
    tables_ref[0] = cosine_ref[...]
    tables_ref[1] = jnp.where(lane % ROPE < ROPE // 2, -sine_ref[...], sine_ref[...])


def pieces_of(value):
    first = value.astype(BF16).astype(F32)
    second = (value - first).astype(BF16).astype(F32)
    third = (value - first - second).astype(BF16).astype(F32)
    return first, second, third


def attend_kernel(scalars_ref, tables_ref, arrived_ref, cache_ref, sent_ref, q_ref, s_ref, p_ref):
    devices = arrived_ref.shape[0]
    places = cache_ref.shape[1]
    rows = q_ref.shape[0] // devices
    half = rows // 2
    for j in range(LATENT_BLOCKS):
        block = arrived_ref[:, j * rows : (j + 1) * rows, :]
        q_ref[:, j * LANES : (j + 1) * LANES] = block.reshape(devices * rows, LANES)
    x = arrived_ref[:, LATENT_BLOCKS * rows :, :].astype(F32).reshape(devices * half, LANES)
    lane = lax.broadcasted_iota(jnp.int32, x.shape, 1)
    partner = jnp.where(
        lane % ROPE < ROPE // 2,
        pltpu.roll(x, LANES - ROPE // 2, 1),
        pltpu.roll(x, ROPE // 2, 1),
    )
    shape3 = (devices, half, LANES)
    turned = x.reshape(shape3) * tables_ref[0][None] + partner.reshape(shape3) * tables_ref[1][None]
    swapped = pltpu.roll(turned.reshape(devices * half, LANES), ROPE, 1).reshape(shape3)
    rope = jnp.stack([turned, swapped], axis=1).reshape(devices * rows, LANES)
    q_ref[:, LATENT:] = rope[:, :ROPE].astype(BF16)

    row = lax.broadcasted_iota(jnp.int32, (devices * rows, TILE), 0) % rows
    limits = jnp.full(row.shape, scalars_ref[0], jnp.int32)
    for t in range(1, DRAFT):
        limits = jnp.where(row >= t * (rows // DRAFT), scalars_ref[t], limits)
    limits = limits - lax.broadcasted_iota(jnp.int32, row.shape, 1)
    top = jnp.full((devices * rows, LANES), negative, F32)
    for i in range(places // TILE):
        scores = lax.dot_general(
            q_ref[...],
            cache_ref[:, i * TILE : (i + 1) * TILE],
            (((1,), (0,)), ((), ())),
            preferred_element_type=F32,
        )
        scores = jnp.where(limits >= i * TILE, scores, negative)
        s_ref[:, i * TILE : (i + 1) * TILE] = scores
        for j in range(TILE // LANES):
            top = jnp.maximum(top, scores[:, j * LANES : (j + 1) * LANES])
    peak = jnp.max(top, axis=1, keepdims=True)
    total = jnp.zeros((devices * rows, LANES), F32)
    for i in range(places // TILE):
        weights = jnp.exp2((s_ref[:, i * TILE : (i + 1) * TILE] - peak) * scale_log2)
        for j in range(TILE // LANES):
            total += weights[:, j * LANES : (j + 1) * LANES]
        p_ref[:, i * TILE : (i + 1) * TILE] = weights.astype(BF16)
    total = jnp.sum(total, axis=1, keepdims=True)
    share = lax.dot_general(
        p_ref[...],
        cache_ref[:LATENT, :],
        (((1,), (1,)), ((), ())),
        preferred_element_type=F32,
    )
    share = share / total
    for j in range(LATENT_BLOCKS):
        block = share[:, j * LANES : (j + 1) * LANES].astype(BF16)
        sent_ref[:, j * rows : (j + 1) * rows, :] = block.reshape(devices, rows, LANES)
    lane = lax.broadcasted_iota(jnp.int32, (devices * rows, LANES), 1)
    stats = jnp.zeros(lane.shape, F32)
    for k, piece in enumerate((*pieces_of(peak), *pieces_of(total))):
        stats = jnp.where(lane % ROPE == k, piece, stats)
    stats = stats.reshape(devices, 2, half, LANES)
    lane = lax.broadcasted_iota(jnp.int32, (devices, half, LANES), 2)
    sent_ref[:, LATENT_BLOCKS * rows :, :] = jnp.where(
        lane < ROPE, stats[:, 0], stats[:, 1]
    ).astype(BF16)


def combine_kernel(arrived_ref, w_uv_ref, sent_ref):
    devices, _, _ = arrived_ref.shape
    heads = w_uv_ref.shape[0]
    rows = DRAFT * heads
    half = rows // 2
    packed = arrived_ref[:, LATENT_BLOCKS * rows :, :].astype(F32)
    stats = jnp.concatenate(
        [packed, pltpu.roll(packed.reshape(devices * half, LANES), ROPE, 1).reshape(packed.shape)],
        axis=1,
    )
    peaks = stats[:, :, 0:1] + stats[:, :, 1:2] + stats[:, :, 2:3]
    parts = stats[:, :, 3:4] + stats[:, :, 4:5] + stats[:, :, 5:6]
    parts = parts * jnp.exp2((peaks - jnp.max(peaks, axis=0, keepdims=True)) * scale_log2)
    parts = parts / jnp.sum(parts, axis=0, keepdims=True)
    blocks = []
    for j in range(LATENT_BLOCKS):
        block = arrived_ref[:, j * rows : (j + 1) * rows, :].astype(F32)
        blocks.append(jnp.sum(block * parts, axis=0))
    attended = jnp.concatenate(blocks, axis=1).astype(BF16)
    row = lax.broadcasted_iota(jnp.int32, (rows, w_uv_ref.shape[2]), 0)
    values = []
    for h in range(heads):
        value = jnp.dot(attended, w_uv_ref[h], preferred_element_type=F32)
        values.append(jnp.where(row % heads == h, value, 0.0))
    values = jnp.concatenate(values, axis=1).astype(BF16)
    token = lax.broadcasted_iota(jnp.int32, (DRAFT, rows), 0)
    member = lax.broadcasted_iota(jnp.int32, (DRAFT, rows), 1) // heads
    pick = (token == member).astype(BF16)
    values = jnp.dot(pick, values, preferred_element_type=F32).astype(BF16)
    for d in range(sent_ref.shape[0]):
        sent_ref[d] = values


def project_kernel(values_ref, w_out_ref, sent_ref):
    devices = values_ref.shape[0]
    blocks = sent_ref.shape[1]
    values = jnp.concatenate([values_ref[d].astype(F32) for d in range(devices)], axis=0)
    mixed = jnp.dot(values.astype(BF16), w_out_ref[...], preferred_element_type=F32)
    width = mixed.shape[1]
    pad = blocks * LANES - width
    mixed = jnp.concatenate([mixed, jnp.zeros((mixed.shape[0], pad), F32)], axis=1)
    sent_ref[...] = mixed.reshape(mixed.shape[0], blocks, LANES).astype(BF16)


def total_kernel(arrived_ref, mixed_ref):
    total = jnp.sum(arrived_ref[...].astype(F32), axis=0)
    for j in range(mixed_ref.shape[1] // LANES):
        mixed_ref[:, j * LANES : (j + 1) * LANES] = total[j : j + 1].astype(BF16)


def limited(mebibytes):
    return pltpu.CompilerParams(vmem_limit_bytes=mebibytes * 1024 * 1024)


def per_device(queries, cache, lengths, offsets, w_uv, w_out):
    heads = queries.shape[2]
    rows = DRAFT * heads
    places = cache.shape[1]
    devices_ctx = lax.axis_size("ctx")
    devices_seq = lax.axis_size("seq")
    message = LATENT_BLOCKS * rows + rows // 2
    positions = lengths[0] - DRAFT + offsets[0]
    sent, _ = pl.pallas_call(
        pack_kernel,
        out_shape=[
            jax.ShapeDtypeStruct((devices_ctx, message, LANES), BF16),
            jax.ShapeDtypeStruct((8, LANES), F32),
        ],
        in_specs=[VMEM],
        out_specs=[VMEM, VMEM],
        compiler_params=limited(4),
        name="pack",
    )(queries)
    arrived = lax.all_to_all(sent, "ctx", 0, 0, tiled=True)
    scalars = positions - lax.axis_index("ctx") * places
    all_rows = devices_ctx * rows
    sent = pl.pallas_call(
        attend_kernel,
        out_shape=jax.ShapeDtypeStruct((devices_ctx, message, LANES), BF16),
        in_specs=[SMEM, VMEM, VMEM, VMEM],
        out_specs=VMEM,
        scratch_shapes=[
            pltpu.VMEM((all_rows, LATENT + ROPE), BF16),
            pltpu.VMEM((all_rows, places), F32),
            pltpu.VMEM((all_rows, places), BF16),
        ],
        compiler_params=limited(24),
        name="attend",
    )(scalars, rotation_tables(positions, rows), arrived, cache[0].T)
    arrived = lax.all_to_all(sent, "ctx", 0, 0, tiled=True)
    sent = pl.pallas_call(
        combine_kernel,
        out_shape=jax.ShapeDtypeStruct((devices_seq, DRAFT, heads * w_uv.shape[2]), BF16),
        in_specs=[VMEM, VMEM],
        out_specs=VMEM,
        compiler_params=limited(8),
        name="combine",
    )(arrived, w_uv)
    every_token = lax.all_to_all(sent, "seq", 0, 0, tiled=True)
    width = w_out.shape[1]
    blocks = -(-width // (LANES * 8)) * 8
    sent = pl.pallas_call(
        project_kernel,
        out_shape=jax.ShapeDtypeStruct((devices_seq * DRAFT, blocks, LANES), BF16),
        in_specs=[VMEM, VMEM],
        out_specs=VMEM,
        compiler_params=limited(8),
        name="project",
    )(every_token, w_out)
    arrived = lax.all_to_all(sent, ("ctx", "head"), 0, 0, tiled=True)
    return pl.pallas_call(
        total_kernel,
        out_shape=jax.ShapeDtypeStruct((1, width), BF16),
        in_specs=[VMEM],
        out_specs=VMEM,
        compiler_params=limited(4),
        name="total",
    )(arrived)


def solution(mesh):
    in_specs = (
        P(("groups", "seq"), None, ("ctx", "head"), None),
        P(("groups", "seq"), "ctx", None),
        P(("groups", "seq")),
        P(("groups", "seq"), None),
        P(("ctx", "head"), None, None),
        P(("ctx", "head"), "seq"),
    )
    out_specs = P(("groups", "ctx", "head"), "seq")
    return jax.shard_map(
        per_device, mesh=mesh, in_specs=in_specs, out_specs=out_specs, check_vma=False
    )
```

```python
import functools
import math

import jax
import jax.numpy as jnp
import numpy as np
from jax import lax
from jax.experimental import pallas as pl
from jax.experimental.pallas import tpu as pltpu
from jax.sharding import PartitionSpec as P

LATENT = 512
ROPE = 64
NOPE = 128
DRAFT = 4
LANES = 128
TILE = 256
CHUNK = 512
STAGGER = 1000

theta = 10000.0
negative = -1e30
scale = (NOPE + ROPE) ** (-0.5)
scale_log2 = scale * math.log2(math.e)

F32 = jnp.float32
BF16 = jnp.bfloat16
VMEM = pl.BlockSpec(memory_space=pltpu.VMEM)
SMEM = pl.BlockSpec(memory_space=pltpu.SMEM)
LATENT_BLOCKS = LATENT // LANES


def packed_angles(positions, rows):
    half = ROPE // 2
    frequency = np.float32(theta ** (-2.0 * np.arange(half) / ROPE))
    by_row = jnp.repeat(positions.astype(F32), rows // DRAFT).reshape(2, rows // 2)
    angles = by_row[:, :, None] * jnp.asarray(np.tile(frequency, 2))
    return jnp.concatenate([angles[0], angles[1]], axis=-1)


def rotation_tables(positions, rows):
    angles = packed_angles(positions, rows)
    return pl.pallas_call(
        tables_kernel,
        out_shape=jax.ShapeDtypeStruct((2, *angles.shape), F32),
        in_specs=[VMEM, VMEM],
        out_specs=VMEM,
        compiler_params=limited(4),
        name="tables",
    )(jnp.cos(angles), jnp.sin(angles))


def pack_kernel(queries_ref, sent_ref, spun_ref):
    @pl.when(lax.axis_index("head") == 0)
    def _():
        spun_ref[...] = lax.fori_loop(
            0, STAGGER, lambda i, x: x * 0.999 + 0.5, jnp.ones(spun_ref.shape, F32)
        )

    rows = jnp.concatenate([queries_ref[0, t].astype(F32) for t in range(DRAFT)], axis=0)
    half = rows.shape[0] // 2
    parts = [rows[:, j * LANES : (j + 1) * LANES] for j in range(LATENT_BLOCKS)]
    rope = rows[:, LATENT : LATENT + ROPE]
    parts.append(jnp.concatenate([rope[:half], rope[half:]], axis=1))
    message = jnp.concatenate(parts, axis=0).astype(BF16)
    for d in range(sent_ref.shape[0]):
        sent_ref[d] = message


def tables_kernel(cosine_ref, sine_ref, tables_ref):
    lane = lax.broadcasted_iota(jnp.int32, cosine_ref.shape, 1)
    tables_ref[0] = cosine_ref[...]
    tables_ref[1] = jnp.where(lane % ROPE < ROPE // 2, -sine_ref[...], sine_ref[...])


def pieces_of(value):
    first = value.astype(BF16).astype(F32)
    second = (value - first).astype(BF16).astype(F32)
    third = (value - first - second).astype(BF16).astype(F32)
    return first, second, third


def attend_kernel(scalars_ref, tables_ref, arrived_ref, cache_ref, sent_ref, q_ref, s_ref, p_ref, held_ref, sems):
    devices = arrived_ref.shape[0]
    places = cache_ref.shape[1]
    rows = q_ref.shape[0] // devices
    half = rows // 2
    copies = []
    for i in range(places // CHUNK):
        at = (slice(None), pl.ds(i * CHUNK, CHUNK))
        copies.append(pltpu.make_async_copy(cache_ref.at[at], held_ref.at[at], sems.at[i]))
        copies[i].start()
    for j in range(LATENT_BLOCKS):
        block = arrived_ref[:, j * rows : (j + 1) * rows, :]
        q_ref[:, j * LANES : (j + 1) * LANES] = block.reshape(devices * rows, LANES)
    x = arrived_ref[:, LATENT_BLOCKS * rows :, :].astype(F32).reshape(devices * half, LANES)
    lane = lax.broadcasted_iota(jnp.int32, x.shape, 1)
    partner = jnp.where(
        lane % ROPE < ROPE // 2,
        pltpu.roll(x, LANES - ROPE // 2, 1),
        pltpu.roll(x, ROPE // 2, 1),
    )
    shape3 = (devices, half, LANES)
    turned = x.reshape(shape3) * tables_ref[0][None] + partner.reshape(shape3) * tables_ref[1][None]
    swapped = pltpu.roll(turned.reshape(devices * half, LANES), ROPE, 1).reshape(shape3)
    rope = jnp.stack([turned, swapped], axis=1).reshape(devices * rows, LANES)
    q_ref[:, LATENT:] = rope[:, :ROPE].astype(BF16)

    row = lax.broadcasted_iota(jnp.int32, (devices * rows, TILE), 0) % rows
    limits = jnp.full(row.shape, scalars_ref[0], jnp.int32)
    for t in range(1, DRAFT):
        limits = jnp.where(row >= t * (rows // DRAFT), scalars_ref[t], limits)
    limits = limits - lax.broadcasted_iota(jnp.int32, row.shape, 1)
    top = jnp.full((devices * rows, LANES), negative, F32)
    for i in range(places // TILE):
        if i * TILE % CHUNK == 0:
            copies[i * TILE // CHUNK].wait()
        scores = lax.dot_general(
            q_ref[...],
            held_ref[:, i * TILE : (i + 1) * TILE],
            (((1,), (0,)), ((), ())),
            preferred_element_type=F32,
        )
        scores = jnp.where(limits >= i * TILE, scores, negative)
        s_ref[:, i * TILE : (i + 1) * TILE] = scores
        for j in range(TILE // LANES):
            top = jnp.maximum(top, scores[:, j * LANES : (j + 1) * LANES])
    peak = jnp.max(top, axis=1, keepdims=True)
    total = jnp.zeros((devices * rows, LANES), F32)
    for i in range(places // TILE):
        weights = jnp.exp2((s_ref[:, i * TILE : (i + 1) * TILE] - peak) * scale_log2)
        for j in range(TILE // LANES):
            total += weights[:, j * LANES : (j + 1) * LANES]
        p_ref[:, i * TILE : (i + 1) * TILE] = weights.astype(BF16)
    total = jnp.sum(total, axis=1, keepdims=True)
    share = lax.dot_general(
        p_ref[...],
        held_ref[:LATENT, :],
        (((1,), (1,)), ((), ())),
        preferred_element_type=F32,
    )
    share = share / total
    for j in range(LATENT_BLOCKS):
        block = share[:, j * LANES : (j + 1) * LANES].astype(BF16)
        sent_ref[:, j * rows : (j + 1) * rows, :] = block.reshape(devices, rows, LANES)
    lane = lax.broadcasted_iota(jnp.int32, (devices * rows, LANES), 1)
    stats = jnp.zeros(lane.shape, F32)
    for k, piece in enumerate((*pieces_of(peak), *pieces_of(total))):
        stats = jnp.where(lane % ROPE == k, piece, stats)
    stats = stats.reshape(devices, 2, half, LANES)
    lane = lax.broadcasted_iota(jnp.int32, (devices, half, LANES), 2)
    sent_ref[:, LATENT_BLOCKS * rows :, :] = jnp.where(
        lane < ROPE, stats[:, 0], stats[:, 1]
    ).astype(BF16)


def combine_kernel(arrived_ref, w_uv_ref, sent_ref):
    devices, _, _ = arrived_ref.shape
    heads = w_uv_ref.shape[0]
    rows = DRAFT * heads
    half = rows // 2
    packed = arrived_ref[:, LATENT_BLOCKS * rows :, :].astype(F32)
    stats = jnp.concatenate(
        [packed, pltpu.roll(packed.reshape(devices * half, LANES), ROPE, 1).reshape(packed.shape)],
        axis=1,
    )
    peaks = stats[:, :, 0:1] + stats[:, :, 1:2] + stats[:, :, 2:3]
    parts = stats[:, :, 3:4] + stats[:, :, 4:5] + stats[:, :, 5:6]
    parts = parts * jnp.exp2((peaks - jnp.max(peaks, axis=0, keepdims=True)) * scale_log2)
    parts = parts / jnp.sum(parts, axis=0, keepdims=True)
    blocks = []
    for j in range(LATENT_BLOCKS):
        block = arrived_ref[:, j * rows : (j + 1) * rows, :].astype(F32)
        blocks.append(jnp.sum(block * parts, axis=0))
    attended = jnp.concatenate(blocks, axis=1).astype(BF16)
    row = lax.broadcasted_iota(jnp.int32, (rows, w_uv_ref.shape[2]), 0)
    values = []
    for h in range(heads):
        value = jnp.dot(attended, w_uv_ref[h], preferred_element_type=F32)
        values.append(jnp.where(row % heads == h, value, 0.0))
    values = jnp.concatenate(values, axis=1).astype(BF16)
    token = lax.broadcasted_iota(jnp.int32, (DRAFT, rows), 0)
    member = lax.broadcasted_iota(jnp.int32, (DRAFT, rows), 1) // heads
    pick = (token == member).astype(BF16)
    values = jnp.dot(pick, values, preferred_element_type=F32).astype(BF16)
    for d in range(sent_ref.shape[0]):
        sent_ref[d] = values


def project_kernel(values_ref, w_out_ref, sent_ref):
    devices = values_ref.shape[0]
    blocks = sent_ref.shape[1]
    values = jnp.concatenate([values_ref[d].astype(F32) for d in range(devices)], axis=0)
    mixed = jnp.dot(values.astype(BF16), w_out_ref[...], preferred_element_type=F32)
    width = mixed.shape[1]
    pad = blocks * LANES - width
    mixed = jnp.concatenate([mixed, jnp.zeros((mixed.shape[0], pad), F32)], axis=1)
    sent_ref[...] = mixed.reshape(mixed.shape[0], blocks, LANES).astype(BF16)


def total_kernel(arrived_ref, mixed_ref):
    total = jnp.sum(arrived_ref[...].astype(F32), axis=0)
    for j in range(mixed_ref.shape[1] // LANES):
        mixed_ref[:, j * LANES : (j + 1) * LANES] = total[j : j + 1].astype(BF16)


def limited(mebibytes):
    return pltpu.CompilerParams(vmem_limit_bytes=mebibytes * 1024 * 1024)


def per_device(queries, cache, lengths, offsets, w_uv, w_out):
    heads = queries.shape[2]
    rows = DRAFT * heads
    places = cache.shape[1]
    devices_ctx = lax.axis_size("ctx")
    devices_seq = lax.axis_size("seq")
    message = LATENT_BLOCKS * rows + rows // 2
    positions = lengths[0] - DRAFT + offsets[0]
    sent, _ = pl.pallas_call(
        pack_kernel,
        out_shape=[
            jax.ShapeDtypeStruct((devices_ctx, message, LANES), BF16),
            jax.ShapeDtypeStruct((8, LANES), F32),
        ],
        in_specs=[VMEM],
        out_specs=[VMEM, VMEM],
        compiler_params=limited(4),
        name="pack",
    )(queries)
    arrived = lax.all_to_all(sent, "ctx", 0, 0, tiled=True)
    scalars = positions - lax.axis_index("ctx") * places
    all_rows = devices_ctx * rows
    sent = pl.pallas_call(
        attend_kernel,
        out_shape=jax.ShapeDtypeStruct((devices_ctx, message, LANES), BF16),
        in_specs=[SMEM, VMEM, VMEM, pl.BlockSpec(memory_space=pltpu.HBM)],
        out_specs=VMEM,
        scratch_shapes=[
            pltpu.VMEM((all_rows, LATENT + ROPE), BF16),
            pltpu.VMEM((all_rows, places), F32),
            pltpu.VMEM((all_rows, places), BF16),
            pltpu.VMEM((LATENT + ROPE, places), BF16),
            pltpu.SemaphoreType.DMA((places // CHUNK,)),
        ],
        compiler_params=limited(52),
        name="attend",
    )(scalars, rotation_tables(positions, rows), arrived, cache[0].T)
    arrived = lax.all_to_all(sent, "ctx", 0, 0, tiled=True)
    sent = pl.pallas_call(
        combine_kernel,
        out_shape=jax.ShapeDtypeStruct((devices_seq, DRAFT, heads * w_uv.shape[2]), BF16),
        in_specs=[VMEM, VMEM],
        out_specs=VMEM,
        compiler_params=limited(8),
        name="combine",
    )(arrived, w_uv)
    every_token = lax.all_to_all(sent, "seq", 0, 0, tiled=True)
    width = w_out.shape[1]
    blocks = -(-width // (LANES * 8)) * 8
    sent = pl.pallas_call(
        project_kernel,
        out_shape=jax.ShapeDtypeStruct((devices_seq * DRAFT, blocks, LANES), BF16),
        in_specs=[VMEM, VMEM],
        out_specs=VMEM,
        compiler_params=limited(8),
        name="project",
    )(every_token, w_out)
    arrived = lax.all_to_all(sent, ("ctx", "head"), 0, 0, tiled=True)
    return pl.pallas_call(
        total_kernel,
        out_shape=jax.ShapeDtypeStruct((1, width), BF16),
        in_specs=[VMEM],
        out_specs=VMEM,
        compiler_params=limited(4),
        name="total",
    )(arrived)


def solution(mesh):
    in_specs = (
        P(("groups", "seq"), None, ("ctx", "head"), None),
        P(("groups", "seq"), "ctx", None),
        P(("groups", "seq")),
        P(("groups", "seq"), None),
        P(("ctx", "head"), None, None),
        P(("ctx", "head"), "seq"),
    )
    out_specs = P(("groups", "ctx", "head"), "seq")
    return jax.shard_map(
        per_device, mesh=mesh, in_specs=in_specs, out_specs=out_specs, check_vma=False
    )
```
